8 devices in a mesh: dp: 1 (over z), tp: 2 (over y), pp: 4 (over x, core).
Axes of the slice: x: 2, y: 2, z: 1, core: 2. Of those that a mesh axis runs over, the one named last changes fastest.
Arguments:
- hidden_in: bfloat16 [12, 3, 384, 2560], P(None, 'dp')
- positions: int32 [12, 3, 384], P(None, 'dp')
- ln_params: float32 [4, 4, 2560], P('pp')
- w_qkv: bfloat16 [4, 2560, 3, 32, 80], P('pp', None, None, 'tp')
- b_qkv: float32 [4, 3, 32, 80], P('pp', None, 'tp')
- w_out: bfloat16 [4, 32, 80, 2560], P('pp', 'tp')
- w_up: bfloat16 [4, 2560, 10240], P('pp', None, 'tp')
- b_up: float32 [4, 10240], P('pp', 'tp')
- w_down: bfloat16 [4, 10240, 2560], P('pp', 'tp')
- b_res: float32 [4, 2, 2560], P('pp')
Outputs:
- output: bfloat16 [4, 12, 3, 384, 2560], P('pp', None, 'dp')
All inputs are finite; a program needn't handle non-finite values.
Results may differ from the reference program's by a relative error of at most 0.0182143.
Values are sent between devices in bfloat16 or wider.
A program may use at most 1 GiB of HBM per device.

```python
import jax
import jax.numpy as jnp
from jax import lax

NUM_STAGES = 4
NUM_MICRO = 12
MICRO_ROWS = 3
SEQ_LEN = 384
D_MODEL = 2560
NUM_HEADS = 32
HEAD_DIM = 80
FF_DIM = 10240


def setup_inputs(seed: int = 0, part: int = 0) -> dict:
    weight_keys = jax.random.split(jax.random.key(seed), 8)
    part_key = jax.random.fold_in(jax.random.key(seed + 1), part)
    data_keys = jax.random.split(part_key, 3)
    act_shape = (NUM_MICRO, MICRO_ROWS, SEQ_LEN, D_MODEL)
    hidden_in = jax.random.normal(data_keys[0], act_shape, jnp.float32).astype(jnp.bfloat16)
    steps_up = jax.random.randint(data_keys[1], (NUM_MICRO, MICRO_ROWS, SEQ_LEN), 1, 4, dtype=jnp.int32)
    starts = jax.random.randint(data_keys[2], (NUM_MICRO, MICRO_ROWS, 1), 0, SEQ_LEN, dtype=jnp.int32)
    positions = (starts + jnp.cumsum(steps_up, axis=-1)).astype(jnp.int32)
    ln_base = jnp.array([1.0, 0.0, 1.0, 0.0], jnp.float32)[None, :, None]
    ln_params = ln_base + 0.3 * jax.random.normal(weight_keys[0], (NUM_STAGES, 4, D_MODEL), jnp.float32)
    w_qkv = (jax.random.normal(weight_keys[1], (NUM_STAGES, D_MODEL, 3, NUM_HEADS, HEAD_DIM), jnp.float32) * D_MODEL ** -0.5).astype(jnp.bfloat16)
    b_qkv = 0.2 * jax.random.normal(weight_keys[2], (NUM_STAGES, 3, NUM_HEADS, HEAD_DIM), jnp.float32)
    w_out = (jax.random.normal(weight_keys[3], (NUM_STAGES, NUM_HEADS, HEAD_DIM, D_MODEL), jnp.float32) * D_MODEL ** -0.5).astype(jnp.bfloat16)
    w_up = (jax.random.normal(weight_keys[4], (NUM_STAGES, D_MODEL, FF_DIM), jnp.float32) * D_MODEL ** -0.5).astype(jnp.bfloat16)
    b_up = 0.5 * jax.random.normal(weight_keys[5], (NUM_STAGES, FF_DIM), jnp.float32)
    w_down = (jax.random.normal(weight_keys[6], (NUM_STAGES, FF_DIM, D_MODEL), jnp.float32) * FF_DIM ** -0.5).astype(jnp.bfloat16)
    b_res = 0.2 * jax.random.normal(weight_keys[7], (NUM_STAGES, 2, D_MODEL), jnp.float32)
    return dict(hidden_in=hidden_in, positions=positions, ln_params=ln_params, w_qkv=w_qkv, b_qkv=b_qkv, w_out=w_out, w_up=w_up, b_up=b_up, w_down=w_down, b_res=b_res)


def layer_norm(hidden, ln_gain, ln_shift):
    hid_f32 = hidden.astype(jnp.float32)
    row_mean = jnp.mean(hid_f32, axis=-1, keepdims=True)
    centred = hid_f32 - row_mean
    row_var = jnp.mean(centred * centred, axis=-1, keepdims=True)
    return (centred * lax.rsqrt(row_var + 1e-5) * ln_gain + ln_shift).astype(jnp.bfloat16)


def block_layer(hidden, pos_rows, layer_w):
    ln_p, w_qkv, b_qkv, w_out, w_up, b_up, w_down, b_res = layer_w
    tokens = MICRO_ROWS * SEQ_LEN
    normed = layer_norm(hidden, ln_p[0], ln_p[1])
    qkv_f = jnp.dot(normed.reshape(tokens, D_MODEL), w_qkv.reshape(D_MODEL, 3 * D_MODEL), preferred_element_type=jnp.float32)
    qkv_h = (qkv_f.reshape(MICRO_ROWS, SEQ_LEN, 3, NUM_HEADS, HEAD_DIM) + b_qkv).astype(jnp.bfloat16)
    query_h = qkv_h[:, :, 0].astype(jnp.float32)
    key_h = qkv_h[:, :, 1].astype(jnp.float32)
    value_h = qkv_h[:, :, 2].astype(jnp.float32)
    scores = jnp.einsum("bqhe,bkhe->bhqk", query_h, key_h) * HEAD_DIM ** -0.5
    head_ids = jnp.arange(NUM_HEADS, dtype=jnp.float32)
    slopes = jnp.exp2(-8.0 * (head_ids + 1.0) / NUM_HEADS)
    rel_pos = (pos_rows[:, :, None] - pos_rows[:, None, :]).astype(jnp.float32)
    scores = scores - slopes[None, :, None, None] * rel_pos[:, None, :, :]
    causal = jnp.arange(SEQ_LEN)[:, None] >= jnp.arange(SEQ_LEN)[None, :]
    scores = jnp.where(causal, scores, -1e30)
    probs_bf = jax.nn.softmax(scores, axis=-1).astype(jnp.bfloat16)
    context = jnp.einsum("bhqk,bkhe->bqhe", probs_bf.astype(jnp.float32), value_h).astype(jnp.bfloat16)
    attn_f = jnp.dot(context.reshape(tokens, D_MODEL), w_out.reshape(D_MODEL, D_MODEL), preferred_element_type=jnp.float32)
    resid_mid = (hidden.astype(jnp.float32) + attn_f.reshape(MICRO_ROWS, SEQ_LEN, D_MODEL) + b_res[0]).astype(jnp.bfloat16)
    normed_mlp = layer_norm(resid_mid, ln_p[2], ln_p[3])
    up_f = jnp.dot(normed_mlp.reshape(tokens, D_MODEL), w_up, preferred_element_type=jnp.float32) + b_up
    gelu_out = jax.nn.gelu(up_f, approximate=True).astype(jnp.bfloat16)
    down_f = jnp.dot(gelu_out, w_down, preferred_element_type=jnp.float32)
    return (resid_mid.astype(jnp.float32) + down_f.reshape(MICRO_ROWS, SEQ_LEN, D_MODEL) + b_res[1]).astype(jnp.bfloat16)


def reference(hidden_in, positions, ln_params, w_qkv, b_qkv, w_out, w_up, b_up, w_down, b_res):
    def layer_step(hidden, layer_w):
        def one_micro(micro_pair):
            return block_layer(micro_pair[0], micro_pair[1], layer_w)
        new_hidden = lax.map(one_micro, (hidden, positions))
        return new_hidden, new_hidden
    _, stage_outs = lax.scan(layer_step, hidden_in, (ln_params, w_qkv, b_qkv, w_out, w_up, b_up, w_down, b_res))
    return stage_outs
```

```python
import functools
import math

import jax
import jax.numpy as jnp
from jax import lax
from jax.experimental import pallas as pl
from jax.experimental.pallas import tpu as pltpu
from jax.sharding import PartitionSpec as P


LAG = 3
ROW_CHUNK = 32


def tie(x, after):
    return (x, after) if after is None else lax.optimization_barrier((x, after))


def normalise_rows(src_ref, gain_ref, shift_ref, dst_ref):
    chunk = math.gcd(src_ref.shape[0], ROW_CHUNK)

    def body(c, carry):
        rows = pl.ds(pl.multiple_of(c * chunk, chunk), chunk)
        x = src_ref[rows, :].astype(jnp.float32)
        centred = x - jnp.mean(x, axis=-1, keepdims=True)
        var = jnp.mean(centred * centred, axis=-1, keepdims=True)
        dst_ref[rows, :] = (centred * lax.rsqrt(var + 1e-5) * gain_ref[...] + shift_ref[...]).astype(jnp.bfloat16)
        return carry

    lax.fori_loop(0, src_ref.shape[0] // chunk, body, 0)


def qkv_kernel(h_ref, gain_ref, shift_ref, w_ref, b_ref, o_ref, a_ref, at_ref):
    @pl.when(pl.program_id(0) == 0)
    def _():
        normalise_rows(h_ref, gain_ref, shift_ref, a_ref)
        for c in range(a_ref.shape[0] // 128):
            at_ref[:, c * 128:(c + 1) * 128] = a_ref[c * 128:(c + 1) * 128, :].T

    acc = jnp.dot(w_ref[...], at_ref[...], preferred_element_type=jnp.float32)
    o_ref[...] = (acc + b_ref[...]).astype(jnp.bfloat16)


def params(n_axes=1):
    return pltpu.CompilerParams(dimension_semantics=("arbitrary",) * n_axes, vmem_limit_bytes=44 * 1024 * 1024)


def cost(rows, depth, cols):
    return pl.CostEstimate(flops=2 * rows * depth * cols, bytes_accessed=2 * depth * cols, transcendentals=0)


def qkv_project(h, gain, shift, w_t, b_col):
    rows, width = h.shape
    cols = w_t.shape[0]
    blk = 384 if cols % 384 == 0 else 96
    whole = lambda shape: pl.BlockSpec(shape, lambda i: (0, 0))
    return pl.pallas_call(
        qkv_kernel,
        grid=(cols // blk,),
        out_shape=jax.ShapeDtypeStruct((cols, rows), jnp.bfloat16),
        in_specs=[whole((rows, width)), whole((1, width)), whole((1, width)),
                  pl.BlockSpec((blk, width), lambda i: (i, 0)), pl.BlockSpec((blk, 1), lambda i: (i, 0))],
        out_specs=pl.BlockSpec((blk, rows), lambda i: (i, 0)),
        scratch_shapes=[pltpu.VMEM((rows, width), jnp.bfloat16), pltpu.VMEM((width, rows), jnp.bfloat16)],
        compiler_params=params(), cost_estimate=cost(rows, width, cols), name="qkv_t",
    )(h, gain, shift, w_t, b_col)


def middle_kernel(n_out, blk, tp_ref, h_ref, mine_ref, their_ref, wo_ref, bo_ref, gain_ref, shift_ref, wu_ref, bu_ref,
                  r_ref, g_ref, ctx_ref, u_ref):
    step = pl.program_id(0)
    half = mine_ref.shape[1]

    @pl.when((step == 0) & (tp_ref[0] == 0))
    def _():
        ctx_ref[:, :half] = mine_ref[...]
        ctx_ref[:, half:] = their_ref[...]

    @pl.when((step == 0) & (tp_ref[0] != 0))
    def _():
        ctx_ref[:, :half] = their_ref[...]
        ctx_ref[:, half:] = mine_ref[...]

    @pl.when(step < n_out)
    def _():
        cols = pl.ds(pl.multiple_of(step * blk, blk), blk)
        attn = jnp.dot(ctx_ref[...], wo_ref[...], preferred_element_type=jnp.float32)
        r_ref[:, cols] = (h_ref[:, cols].astype(jnp.float32) + attn + bo_ref[...]).astype(jnp.bfloat16)

    @pl.when(step == n_out - 1)
    def _():
        normalise_rows(r_ref, gain_ref, shift_ref, u_ref)

    @pl.when(step >= n_out)
    def _():
        up = jnp.dot(u_ref[...], wu_ref[...], preferred_element_type=jnp.float32) + bu_ref[...]
        g_ref[...] = jax.nn.gelu(up, approximate=True).astype(jnp.bfloat16)


def middle_block(tp_id, h, ctx_m, ctx_t, w_o, b_o, gain, shift, w_up, b_up):
    rows, width = h.shape
    ff = w_up.shape[1]
    blk = 512 if width % 512 == 0 else 128
    n_out, n_up = width // blk, ff // blk
    half = ctx_m.shape[1]
    whole = lambda shape: pl.BlockSpec(shape, lambda i: (0, 0))
    at_out = lambda i: (0, jnp.minimum(i, n_out - 1))
    at_up = lambda i: (0, jnp.maximum(i - n_out, 0))
    return pl.pallas_call(
        functools.partial(middle_kernel, n_out, blk),
        grid=(n_out + n_up,),
        out_shape=(jax.ShapeDtypeStruct((rows, width), jnp.bfloat16), jax.ShapeDtypeStruct((rows, ff), jnp.bfloat16)),
        in_specs=[pl.BlockSpec(memory_space=pltpu.SMEM), whole((rows, width)), whole((rows, half)), whole((rows, half)),
                  pl.BlockSpec((width, blk), at_out), pl.BlockSpec((1, blk), at_out), whole((1, width)), whole((1, width)),
                  pl.BlockSpec((width, blk), at_up), pl.BlockSpec((1, blk), at_up)],
        out_specs=(whole((rows, width)), pl.BlockSpec((rows, blk), at_up)),
        scratch_shapes=[pltpu.VMEM((rows, 2 * half), jnp.bfloat16), pltpu.VMEM((rows, width), jnp.bfloat16)],
        compiler_params=params(), cost_estimate=cost(rows, width, width + ff), name="middle",
    )(tp_id, h, ctx_m, ctx_t, w_o, b_o, gain, shift, w_up, b_up)


def down_kernel(g_ref, w_ref, o_ref):
    o_ref[...] = jnp.dot(g_ref[...], w_ref[...], preferred_element_type=jnp.float32).astype(jnp.bfloat16)


def down_project(g, w_down):
    rows, ff = g.shape
    width = w_down.shape[1]
    blk = 256 if width % 256 == 0 else 64
    return pl.pallas_call(
        down_kernel,
        grid=(width // blk,),
        out_shape=jax.ShapeDtypeStruct((rows, width), jnp.bfloat16),
        in_specs=[pl.BlockSpec((rows, ff), lambda i: (0, 0)), pl.BlockSpec((ff, blk), lambda i: (0, i))],
        out_specs=pl.BlockSpec((rows, blk), lambda i: (0, i)),
        compiler_params=params(), cost_estimate=cost(rows, ff, width), name="down",
    )(g, w_down)


def attention_kernel(heads_step, head_dim, blk, slope_ref, pos_col_ref, pos_row_ref, q_ref, k_ref, v_ref, o_ref, rel_ref, out_ref):
    step = pl.program_id(0)
    seq = q_ref.shape[1]

    @pl.when(step == 0)
    def _():
        rel = (pos_row_ref[...] - pos_col_ref[...]).astype(jnp.float32)
        key_id = lax.broadcasted_iota(jnp.int32, (seq, seq), 0)
        query_id = lax.broadcasted_iota(jnp.int32, (seq, seq), 1)
        rel_ref[...] = jnp.where(key_id <= query_id, rel, 1e33)

    scale = head_dim ** -0.5
    for h in range(heads_step):
        slope = slope_ref[step * heads_step + h]
        rows = pl.ds(h * head_dim, head_dim)
        for qb in range(seq // blk):
            n_key = (qb + 1) * blk
            cols = pl.ds(qb * blk, blk)
            s = lax.dot_general(k_ref[rows, 0:n_key], q_ref[rows, cols], (((0,), (0,)), ((), ())),
                                preferred_element_type=jnp.float32)
            s = s * scale - slope * rel_ref[0:n_key, cols]
            p = jnp.exp(s - jnp.max(s, axis=0, keepdims=True))
            p = (p / jnp.sum(p, axis=0, keepdims=True)).astype(jnp.bfloat16)
            c = jnp.dot(v_ref[rows, 0:n_key], p, preferred_element_type=jnp.float32)
            out_ref[rows, cols] = c
    o_ref[...] = out_ref[...].T.astype(jnp.bfloat16)


def attention(qkv_t, pos, slopes, n_heads, head_dim, heads_step, blk):
    seq = pos.shape[0]
    steps = n_heads // heads_step
    rows = heads_step * head_dim
    block = lambda part: pl.BlockSpec((rows, seq), lambda i, part=part: (part * steps + i, 0))
    return pl.pallas_call(
        functools.partial(attention_kernel, heads_step, head_dim, blk),
        grid=(steps,),
        out_shape=jax.ShapeDtypeStruct((seq, n_heads * head_dim), jnp.bfloat16),
        in_specs=[
            pl.BlockSpec(memory_space=pltpu.SMEM),
            pl.BlockSpec((seq, 1), lambda i: (0, 0)),
            pl.BlockSpec((1, seq), lambda i: (0, 0)),
            block(0), block(1), block(2),
        ],
        out_specs=pl.BlockSpec((seq, rows), lambda i: (0, i)),
        scratch_shapes=[pltpu.VMEM((seq, seq), jnp.float32), pltpu.VMEM((rows, seq), jnp.float32)],
        compiler_params=pltpu.CompilerParams(dimension_semantics=("arbitrary",), vmem_limit_bytes=16 * 1024 * 1024),
        cost_estimate=pl.CostEstimate(flops=n_heads * seq * seq * 512 * 2, bytes_accessed=8 * n_heads * head_dim * seq,
                                      transcendentals=n_heads * seq * seq),
        name="attention_t",
    )(slopes, pos[:, None], pos[None, :], qkv_t, qkv_t, qkv_t)


def solution(mesh):
    tp_size = mesh.shape["tp"]
    pp_size = mesh.shape["pp"]
    assert tp_size == 2

    def stage_body(hidden_in, positions, ln_params, w_qkv, b_qkv, w_out, w_up, b_up, w_down, b_res):
        stage_id = lax.axis_index("pp")
        tp_id = lax.axis_index("tp")
        n_micro, n_rows, seq, width = hidden_in.shape
        n_local, head_dim = w_qkv.shape[3], w_qkv.shape[4]
        n_units = n_micro * n_rows
        local_w = n_local * head_dim
        head_ids = (tp_id * n_local + jnp.arange(n_local)).astype(jnp.float32)
        slopes = jnp.exp2(-8.0 * (head_ids + 1.0) / (n_local * tp_size))
        x_in = hidden_in.reshape(n_units, seq, width)
        pos_in = positions.reshape(n_units, seq)
        ln_p = ln_params[0]
        w_qkv_t = jnp.transpose(w_qkv[0], (1, 2, 3, 0)).reshape(3 * local_w, width)
        b_qkv_c = b_qkv[0].reshape(3 * local_w, 1)
        w_up_l, b_up_l, w_down_l, b_r = w_up[0], b_up, w_down[0], b_res[0]
        tp_arr = tp_id.astype(jnp.int32).reshape(1)
        both = [(t * pp_size + s, (1 - t) * pp_size + s) for s in range(pp_size) for t in range(tp_size)]
        w_mine = w_out[0].reshape(local_w, width)
        w_their = lax.ppermute(w_mine, ("tp", "pp"), perm=both)
        w_o = jnp.concatenate([jnp.where(tp_id == 0, w_mine, w_their), jnp.where(tp_id == 0, w_their, w_mine)], axis=0)

        def active(i):
            return [s for s in range(pp_size) if 0 <= i - LAG * s < n_units]

        def swap(x, i):
            perm = [(t * pp_size + s, (1 - t) * pp_size + s) for s in active(i) for t in range(tp_size)]
            return lax.ppermute(x, ("tp", "pp"), perm=perm)

        def front(i, after):
            fresh = x_in[min(i, n_units - 1)]
            h = fresh if i < LAG else jnp.where(stage_id == 0, fresh, sent.pop(i - LAG))
            h, _ = tie(h, after)
            unit = jnp.clip(i - LAG * stage_id, 0, n_units - 1)
            pos = lax.dynamic_index_in_dim(pos_in, unit, 0, keepdims=False)
            qkv_t = qkv_project(h, ln_p[0:1], ln_p[1:2], w_qkv_t, b_qkv_c)
            ctx_m = attention(qkv_t, pos, slopes, n_local, head_dim, math.gcd(n_local, 8), min(seq, 128))
            return h, ctx_m, swap(ctx_m, i)

        def middle(h, ctx_m, ctx_t, after):
            ctx_m, _ = tie(ctx_m, after)
            return middle_block(tp_arr, h, ctx_m, ctx_t, w_o, b_r[0:1], ln_p[2:3], ln_p[3:4], w_up_l, b_up_l)

        def down(i, g, after):
            g, _ = tie(g, after)
            part_m = down_project(g, w_down_l)
            return part_m, swap(part_m, i)

        def finish(i, acts, r, part_m, part_t, after):
            r, _ = tie(r, after)
            out = (r.astype(jnp.float32) + (part_m.astype(jnp.float32) + part_t.astype(jnp.float32)) + b_r[1]).astype(jnp.bfloat16)
            shift = [(t * pp_size + s, t * pp_size + s + 1) for s in active(i) if s + 1 < pp_size for t in range(tp_size)]
            if shift:
                sent[i] = lax.ppermute(out, ("tp", "pp"), perm=shift)
            unit = i - LAG * stage_id
            unit_c = jnp.clip(unit, 0, n_units - 1)
            stored = out
            if i >= n_units:
                prev = lax.dynamic_index_in_dim(acts, unit_c, 0, keepdims=False)
                stored = jnp.where(unit < n_units, out, prev)
            return lax.dynamic_update_index_in_dim(acts, stored, unit_c, 0), out

        n_slots = n_units + LAG * (pp_size - 1)
        acts = jnp.zeros((n_units, seq, width), jnp.bfloat16)
        sent, fronts, mids, parts = {}, {}, {}, {}
        last = None
        for i in range(n_slots + 2):
            if i < n_slots:
                fronts[i] = front(i, last)
                last = fronts[i][1]
            if 0 <= i - 1 < n_slots:
                mids[i - 1] = middle(*fronts.pop(i - 1), last)
                last = mids[i - 1][1]
            if i - 2 >= 0:
                acts, last = finish(i - 2, acts, mids.pop(i - 2)[0], *parts.pop(i - 2), last)
            if 0 <= i - 1 < n_slots:
                parts[i - 1] = down(i - 1, mids[i - 1][1], last)
                last = parts[i - 1][0]
        return acts.reshape(1, n_micro, n_rows, seq, width)

    in_specs = (P(None, "dp", None, None), P(None, "dp", None), P("pp", None, None), P("pp", None, None, "tp", None), P("pp", None, "tp", None), P("pp", "tp", None, None), P("pp", None, "tp"), P("pp", "tp"), P("pp", "tp", None), P("pp", None, None))
    return jax.shard_map(stage_body, mesh=mesh, in_specs=in_specs, out_specs=P("pp", None, "dp", None, None), check_vma=False)
```

```python
import functools
import math

import jax
import jax.numpy as jnp
from jax import lax
from jax.experimental import pallas as pl
from jax.experimental.pallas import tpu as pltpu
from jax.sharding import PartitionSpec as P


LAG = 3
ROW_CHUNK = 32


def tie(x, after):
    return (x, after) if after is None else lax.optimization_barrier((x, after))


def normalise_rows(src_ref, gain_ref, shift_ref, dst_ref):
    chunk = math.gcd(src_ref.shape[0], ROW_CHUNK)

    def body(c, carry):
        rows = pl.ds(pl.multiple_of(c * chunk, chunk), chunk)
        x = src_ref[rows, :].astype(jnp.float32)
        centred = x - jnp.mean(x, axis=-1, keepdims=True)
        var = jnp.mean(centred * centred, axis=-1, keepdims=True)
        dst_ref[rows, :] = (centred * lax.rsqrt(var + 1e-5) * gain_ref[...] + shift_ref[...]).astype(jnp.bfloat16)
        return carry

    lax.fori_loop(0, src_ref.shape[0] // chunk, body, 0)


def qkv_kernel(h_ref, gain_ref, shift_ref, w_ref, b_ref, o_ref, a_ref, at_ref):
    @pl.when(pl.program_id(0) == 0)
    def _():
        normalise_rows(h_ref, gain_ref, shift_ref, a_ref)
        for c in range(a_ref.shape[0] // 128):
            at_ref[:, c * 128:(c + 1) * 128] = a_ref[c * 128:(c + 1) * 128, :].T

    acc = jnp.dot(w_ref[...], at_ref[...], preferred_element_type=jnp.float32)
    o_ref[...] = (acc + b_ref[...]).astype(jnp.bfloat16)


def params(mib):
    return pltpu.CompilerParams(dimension_semantics=("arbitrary",), vmem_limit_bytes=mib * 1024 * 1024)


def cost(rows, depth, cols):
    return pl.CostEstimate(flops=2 * rows * depth * cols, bytes_accessed=2 * depth * cols, transcendentals=0)


def qkv_project(h, gain, shift, w_t, b_col):
    rows, width = h.shape
    cols = w_t.shape[0]
    blk = 768 if cols % 768 == 0 else 96
    whole = lambda shape: pl.BlockSpec(shape, lambda i: (0, 0))
    return pl.pallas_call(
        qkv_kernel,
        grid=(cols // blk,),
        out_shape=jax.ShapeDtypeStruct((cols, rows), jnp.bfloat16),
        in_specs=[whole((rows, width)), whole((1, width)), whole((1, width)),
                  pl.BlockSpec((blk, width), lambda i: (i, 0)), pl.BlockSpec((blk, 1), lambda i: (i, 0))],
        out_specs=pl.BlockSpec((blk, rows), lambda i: (i, 0)),
        scratch_shapes=[pltpu.VMEM((rows, width), jnp.bfloat16), pltpu.VMEM((width, rows), jnp.bfloat16)],
        compiler_params=params(36), cost_estimate=cost(rows, width, cols), name="qkv_t",
    )(h, gain, shift, w_t, b_col)


def middle_kernel(n_out, blk, tp_ref, h_ref, mine_ref, their_ref, wo_ref, bo_ref, gain_ref, shift_ref, wu_ref, bu_ref,
                  r_ref, g_ref, ctx_ref, u_ref):
    step = pl.program_id(0)
    half = mine_ref.shape[1]

    @pl.when((step == 0) & (tp_ref[0] == 0))
    def _():
        ctx_ref[:, :half] = mine_ref[...]
        ctx_ref[:, half:] = their_ref[...]

    @pl.when((step == 0) & (tp_ref[0] != 0))
    def _():
        ctx_ref[:, :half] = their_ref[...]
        ctx_ref[:, half:] = mine_ref[...]

    @pl.when(step < n_out)
    def _():
        cols = pl.ds(pl.multiple_of(step * blk, blk), blk)
        attn = jnp.dot(ctx_ref[...], wo_ref[...], preferred_element_type=jnp.float32)
        r_ref[:, cols] = (h_ref[:, cols].astype(jnp.float32) + attn + bo_ref[...]).astype(jnp.bfloat16)

    @pl.when(step == n_out - 1)
    def _():
        normalise_rows(r_ref, gain_ref, shift_ref, u_ref)

    @pl.when(step >= n_out)
    def _():
        up = jnp.dot(u_ref[...], wu_ref[...], preferred_element_type=jnp.float32) + bu_ref[...]
        g_ref[...] = jax.nn.gelu(up, approximate=True).astype(jnp.bfloat16)


def middle_block(tp_id, h, ctx_m, ctx_t, w_o, b_o, gain, shift, w_up, b_up):
    rows, width = h.shape
    ff = w_up.shape[1]
    blk = 1280 if width % 1280 == 0 and ff % 1280 == 0 else 128
    n_out, n_up = width // blk, ff // blk
    half = ctx_m.shape[1]
    whole = lambda shape: pl.BlockSpec(shape, lambda i: (0, 0))
    at_out = lambda i: (0, jnp.minimum(i, n_out - 1))
    at_up = lambda i: (0, jnp.maximum(i - n_out, 0))
    return pl.pallas_call(
        functools.partial(middle_kernel, n_out, blk),
        grid=(n_out + n_up,),
        out_shape=(jax.ShapeDtypeStruct((rows, width), jnp.bfloat16), jax.ShapeDtypeStruct((rows, ff), jnp.bfloat16)),
        in_specs=[pl.BlockSpec(memory_space=pltpu.SMEM), whole((rows, width)), whole((rows, half)), whole((rows, half)),
                  pl.BlockSpec((width, blk), at_out), pl.BlockSpec((1, blk), at_out), whole((1, width)), whole((1, width)),
                  pl.BlockSpec((width, blk), at_up), pl.BlockSpec((1, blk), at_up)],
        out_specs=(whole((rows, width)), pl.BlockSpec((rows, blk), at_up)),
        scratch_shapes=[pltpu.VMEM((rows, 2 * half), jnp.bfloat16), pltpu.VMEM((rows, width), jnp.bfloat16)],
        compiler_params=params(58), cost_estimate=cost(rows, width, width + ff), name="middle",
    )(tp_id, h, ctx_m, ctx_t, w_o, b_o, gain, shift, w_up, b_up)


def down_kernel(g_ref, w_ref, o_ref):
    o_ref[...] = jnp.dot(g_ref[...], w_ref[...], preferred_element_type=jnp.float32).astype(jnp.bfloat16)


def down_project(g, w_down):
    rows, ff = g.shape
    width = w_down.shape[1]
    blk = 512 if width % 512 == 0 else 64
    return pl.pallas_call(
        down_kernel,
        grid=(width // blk,),
        out_shape=jax.ShapeDtypeStruct((rows, width), jnp.bfloat16),
        in_specs=[pl.BlockSpec((rows, ff), lambda i: (0, 0)), pl.BlockSpec((ff, blk), lambda i: (0, i))],
        out_specs=pl.BlockSpec((rows, blk), lambda i: (0, i)),
        compiler_params=params(36), cost_estimate=cost(rows, ff, width), name="down",
    )(g, w_down)


def attention_kernel(heads_step, head_dim, blk, slope_ref, pos_col_ref, pos_row_ref, q_ref, k_ref, v_ref, o_ref, rel_ref, out_ref):
    step = pl.program_id(0)
    seq = q_ref.shape[1]

    @pl.when(step == 0)
    def _():
        rel = (pos_row_ref[...] - pos_col_ref[...]).astype(jnp.float32)
        key_id = lax.broadcasted_iota(jnp.int32, (seq, seq), 0)
        query_id = lax.broadcasted_iota(jnp.int32, (seq, seq), 1)
        rel_ref[...] = jnp.where(key_id <= query_id, rel, 1e33)

    scale = head_dim ** -0.5
    for h in range(heads_step):
        slope = slope_ref[step * heads_step + h]
        rows = pl.ds(h * head_dim, head_dim)
        for qb in range(seq // blk):
            n_key = (qb + 1) * blk
            cols = pl.ds(qb * blk, blk)
            s = lax.dot_general(k_ref[rows, 0:n_key], q_ref[rows, cols], (((0,), (0,)), ((), ())),
                                preferred_element_type=jnp.float32)
            s = s * scale - slope * rel_ref[0:n_key, cols]
            p = jnp.exp(s - jnp.max(s, axis=0, keepdims=True))
            p = (p / jnp.sum(p, axis=0, keepdims=True)).astype(jnp.bfloat16)
            c = jnp.dot(v_ref[rows, 0:n_key], p, preferred_element_type=jnp.float32)
            out_ref[rows, cols] = c
    o_ref[...] = out_ref[...].T.astype(jnp.bfloat16)


def attention(qkv_t, pos, slopes, n_heads, head_dim, heads_step, blk):
    seq = pos.shape[0]
    steps = n_heads // heads_step
    rows = heads_step * head_dim
    block = lambda part: pl.BlockSpec((rows, seq), lambda i, part=part: (part * steps + i, 0))
    return pl.pallas_call(
        functools.partial(attention_kernel, heads_step, head_dim, blk),
        grid=(steps,),
        out_shape=jax.ShapeDtypeStruct((seq, n_heads * head_dim), jnp.bfloat16),
        in_specs=[
            pl.BlockSpec(memory_space=pltpu.SMEM),
            pl.BlockSpec((seq, 1), lambda i: (0, 0)),
            pl.BlockSpec((1, seq), lambda i: (0, 0)),
            block(0), block(1), block(2),
        ],
        out_specs=pl.BlockSpec((seq, rows), lambda i: (0, i)),
        scratch_shapes=[pltpu.VMEM((seq, seq), jnp.float32), pltpu.VMEM((rows, seq), jnp.float32)],
        compiler_params=pltpu.CompilerParams(dimension_semantics=("arbitrary",), vmem_limit_bytes=16 * 1024 * 1024),
        cost_estimate=pl.CostEstimate(flops=n_heads * seq * seq * 512 * 2, bytes_accessed=8 * n_heads * head_dim * seq,
                                      transcendentals=n_heads * seq * seq),
        name="attention_t",
    )(slopes, pos[:, None], pos[None, :], qkv_t, qkv_t, qkv_t)


def solution(mesh):
    tp_size = mesh.shape["tp"]
    pp_size = mesh.shape["pp"]
    assert tp_size == 2

    def stage_body(hidden_in, positions, ln_params, w_qkv, b_qkv, w_out, w_up, b_up, w_down, b_res):
        stage_id = lax.axis_index("pp")
        tp_id = lax.axis_index("tp")
        n_micro, n_rows, seq, width = hidden_in.shape
        n_local, head_dim = w_qkv.shape[3], w_qkv.shape[4]
        n_units = n_micro * n_rows
        local_w = n_local * head_dim
        head_ids = (tp_id * n_local + jnp.arange(n_local)).astype(jnp.float32)
        slopes = jnp.exp2(-8.0 * (head_ids + 1.0) / (n_local * tp_size))
        x_in = hidden_in.reshape(n_units, seq, width)
        pos_in = positions.reshape(n_units, seq)
        ln_p = ln_params[0]
        w_qkv_t = jnp.transpose(w_qkv[0], (1, 2, 3, 0)).reshape(3 * local_w, width)
        b_qkv_c = b_qkv[0].reshape(3 * local_w, 1)
        w_up_l, b_up_l, w_down_l, b_r = w_up[0], b_up, w_down[0], b_res[0]
        tp_arr = tp_id.astype(jnp.int32).reshape(1)
        both = [(t * pp_size + s, (1 - t) * pp_size + s) for s in range(pp_size) for t in range(tp_size)]
        w_mine = w_out[0].reshape(local_w, width)
        w_their = lax.ppermute(w_mine, ("tp", "pp"), perm=both)
        w_o = jnp.concatenate([jnp.where(tp_id == 0, w_mine, w_their), jnp.where(tp_id == 0, w_their, w_mine)], axis=0)

        def active(i):
            return [s for s in range(pp_size) if 0 <= i - LAG * s < n_units]

        def swap(x, i):
            perm = [(t * pp_size + s, (1 - t) * pp_size + s) for s in active(i) for t in range(tp_size)]
            return lax.ppermute(x, ("tp", "pp"), perm=perm)

        def front(i, after):
            fresh = x_in[min(i, n_units - 1)]
            h = fresh if i < LAG else jnp.where(stage_id == 0, fresh, sent.pop(i - LAG))
            h, _ = tie(h, after)
            unit = jnp.clip(i - LAG * stage_id, 0, n_units - 1)
            pos = lax.dynamic_index_in_dim(pos_in, unit, 0, keepdims=False)
            qkv_t = qkv_project(h, ln_p[0:1], ln_p[1:2], w_qkv_t, b_qkv_c)
            ctx_m = attention(qkv_t, pos, slopes, n_local, head_dim, math.gcd(n_local, 8), min(seq, 128))
            return h, ctx_m, swap(ctx_m, i)

        def middle(h, ctx_m, ctx_t, after):
            ctx_m, _ = tie(ctx_m, after)
            return middle_block(tp_arr, h, ctx_m, ctx_t, w_o, b_r[0:1], ln_p[2:3], ln_p[3:4], w_up_l, b_up_l)

        def down(i, g, after):
            g, _ = tie(g, after)
            part_m = down_project(g, w_down_l)
            return part_m, swap(part_m, i)

        def finish(i, acts, r, part_m, part_t, after):
            r, _ = tie(r, after)
            out = (r.astype(jnp.float32) + (part_m.astype(jnp.float32) + part_t.astype(jnp.float32)) + b_r[1]).astype(jnp.bfloat16)
            shift = [(t * pp_size + s, t * pp_size + s + 1) for s in active(i) if s + 1 < pp_size for t in range(tp_size)]
            if shift:
                sent[i] = lax.ppermute(out, ("tp", "pp"), perm=shift)
            unit = i - LAG * stage_id
            unit_c = jnp.clip(unit, 0, n_units - 1)
            stored = out
            if i >= n_units:
                prev = lax.dynamic_index_in_dim(acts, unit_c, 0, keepdims=False)
                stored = jnp.where(unit < n_units, out, prev)
            return lax.dynamic_update_index_in_dim(acts, stored, unit_c, 0), out

        n_slots = n_units + LAG * (pp_size - 1)
        acts = jnp.zeros((n_units, seq, width), jnp.bfloat16)
        sent, fronts, mids, parts = {}, {}, {}, {}
        last = None
        for i in range(n_slots + 2):
            if i < n_slots:
                fronts[i] = front(i, last)
                last = fronts[i][1]
            if 0 <= i - 1 < n_slots:
                mids[i - 1] = middle(*fronts.pop(i - 1), last)
                last = mids[i - 1][1]
            if i - 2 >= 0:
                acts, last = finish(i - 2, acts, mids.pop(i - 2)[0], *parts.pop(i - 2), last)
            if 0 <= i - 1 < n_slots:
                parts[i - 1] = down(i - 1, mids[i - 1][1], last)
                last = parts[i - 1][0]
        return acts.reshape(1, n_micro, n_rows, seq, width)

    in_specs = (P(None, "dp", None, None), P(None, "dp", None), P("pp", None, None), P("pp", None, None, "tp", None), P("pp", None, "tp", None), P("pp", "tp", None, None), P("pp", None, "tp"), P("pp", "tp"), P("pp", "tp", None), P("pp", None, None))
    return jax.shard_map(stage_body, mesh=mesh, in_specs=in_specs, out_specs=P("pp", None, "dp", None, None), check_vma=False)
```
